16 devices in a mesh: dp: 2 (over y, z), tp: 8 (over x, core).
Axes of the slice: x: 4, y: 2, z: 1, core: 2. Of those that a mesh axis runs over, the one named last changes fastest.
The devices are a block of a 4x4x8 slice.
Arguments:
- hidden: bfloat16 [32768, 1280], P(('dp', 'tp')), parts along dimension 0
- ln_gain: float32 [1280], replicated
- ln_bias: float32 [1280], replicated
- embed: bfloat16 [16384, 1280], P('tp')
- targets: int32 [32768], P(('dp', 'tp')), parts along dimension 0
- loss_mask: int32 [32768], P(('dp', 'tp')), parts along dimension 0
Outputs:
- output 1: float32 [32768], P(('dp', 'tp')), parts along dimension 0
- output 2: float32 [2], P('dp'), parts along dimension 0
- output 3: bfloat16 [32768, 1280], P(('dp', 'tp')), parts along dimension 0
- output 4: float32 [32768, 1280], P(('dp', 'tp')), parts along dimension 0
- output 5: float32 [2560], P('dp'), parts along dimension 0
- output 6: float32 [2560], P('dp'), parts along dimension 0
There are 2 independent parts. The reference program is written for one: setup_inputs(seed, part) draws one part's arguments, and reference() takes and returns one part's arrays. A program takes and returns all parts, laid end to end along the dimension named above; an argument that names none is the same for every part.
All inputs are finite; a program needn't handle non-finite values.
Results may differ from the reference program's by a relative error of at most 0.001.
Values are sent between devices in bfloat16 or wider.
A program may use at most 768 MiB of HBM per device.

```python
import jax
import jax.numpy as jnp
from jax import lax

TOKENS_DEV = 2048
GROUP_SIZE = 8
MODEL_DIM = 1280
VOCAB_SIZE = 16384
LN_EPS = 1e-5


def setup_inputs(seed: int = 0, part: int = 0) -> dict:
    seq_len = GROUP_SIZE * TOKENS_DEV
    part_keys = jax.random.split(jax.random.fold_in(jax.random.key(seed), part), 4)
    shared_keys = jax.random.split(jax.random.key(seed + 1), 3)
    embed_scale = 2.5 * MODEL_DIM ** -0.5
    hidden = jax.random.normal(part_keys[0], (seq_len, MODEL_DIM), jnp.float32).astype(jnp.bfloat16)
    ln_gain = 1.0 + 0.3 * jax.random.normal(shared_keys[0], (MODEL_DIM,), jnp.float32)
    ln_bias = 0.3 * jax.random.normal(shared_keys[1], (MODEL_DIM,), jnp.float32)
    embed = (embed_scale * jax.random.normal(shared_keys[2], (VOCAB_SIZE, MODEL_DIM), jnp.float32)).astype(jnp.bfloat16)
    targets = jax.random.randint(part_keys[1], (seq_len,), 0, VOCAB_SIZE, dtype=jnp.int32)
    shard_rate = jax.random.randint(part_keys[2], (GROUP_SIZE, 1), 40, 96, dtype=jnp.int32)
    draws = jax.random.randint(part_keys[3], (GROUP_SIZE, TOKENS_DEV), 0, 100, dtype=jnp.int32)
    loss_mask = (draws < shard_rate).astype(jnp.int32).reshape(seq_len)
    return {'hidden': hidden, 'ln_gain': ln_gain, 'ln_bias': ln_bias, 'embed': embed, 'targets': targets, 'loss_mask': loss_mask}


def normalize(hidden):
    h_f32 = hidden.astype(jnp.float32)
    centred = h_f32 - jnp.mean(h_f32, axis=-1, keepdims=True)
    inv_std = lax.rsqrt(jnp.mean(centred * centred, axis=-1, keepdims=True) + LN_EPS)
    return centred * inv_std, inv_std


def reference(hidden, ln_gain, ln_bias, embed, targets, loss_mask):
    seq_len = GROUP_SIZE * TOKENS_DEV
    x_hat, inv_std = normalize(hidden)
    normed = (x_hat * ln_gain + ln_bias).astype(jnp.bfloat16)
    weights = loss_mask.astype(jnp.float32)
    count = jnp.sum(weights)
    vocab_ids = jnp.arange(VOCAB_SIZE, dtype=jnp.int32)

    def block_step(embed_acc, block):
        x_blk, t_blk, w_blk = block
        logits = jnp.dot(x_blk, embed.T, preferred_element_type=jnp.float32)
        row_max = jnp.max(logits, axis=-1, keepdims=True)
        log_norm = row_max[:, 0] + jnp.log(jnp.sum(jnp.exp(logits - row_max), axis=-1))
        onehot = (vocab_ids[None, :] == t_blk[:, None]).astype(jnp.float32)
        t_logit = jnp.sum(logits * onehot, axis=-1)
        loss_blk = (log_norm - t_logit) * w_blk
        d_logits = ((jnp.exp(logits - log_norm[:, None]) - onehot) * (w_blk / count)[:, None]).astype(jnp.bfloat16)
        embed_acc = embed_acc + jnp.dot(d_logits.T, x_blk, preferred_element_type=jnp.float32)
        d_x = jnp.dot(d_logits, embed, preferred_element_type=jnp.float32)
        return embed_acc, (loss_blk, d_x)

    blocks = (normed.reshape(GROUP_SIZE, TOKENS_DEV, MODEL_DIM), targets.reshape(GROUP_SIZE, TOKENS_DEV), weights.reshape(GROUP_SIZE, TOKENS_DEV))
    d_embed, outs = lax.scan(block_step, jnp.zeros((VOCAB_SIZE, MODEL_DIM), jnp.float32), blocks)
    loss = outs[0].reshape(seq_len)
    d_normed = outs[1].reshape(seq_len, MODEL_DIM)
    mean_loss = jnp.sum(loss) / count
    d_gain = jnp.sum(d_normed * x_hat, axis=0)
    d_bias = jnp.sum(d_normed, axis=0)
    d_xhat = d_normed * ln_gain
    centre_term = jnp.mean(d_xhat, axis=-1, keepdims=True)
    proj_term = jnp.mean(d_xhat * x_hat, axis=-1, keepdims=True)
    d_hidden = (inv_std * (d_xhat - centre_term - x_hat * proj_term)).astype(jnp.bfloat16)
    return loss, mean_loss.reshape(1), d_hidden, d_embed, d_gain, d_bias
```

```python
import functools

import jax
import jax.numpy as jnp
from jax import lax
from jax.experimental import pallas as pl
from jax.experimental.pallas import tpu as pltpu
from jax.sharding import PartitionSpec as P


LN_EPS = 1e-5
F32 = jnp.float32
BF16 = jnp.bfloat16
LANES = 128
VMEM_LIMIT = 62 << 20
PIECES = 4
TOKEN_CHUNKS = 2
MIN_GATHER = 1 << 20


def params():
    return pltpu.CompilerParams(vmem_limit_bytes=VMEM_LIMIT, dimension_semantics=('arbitrary',))


def cost(matmuls, rows, cols, depth, extra):
    return pl.CostEstimate(flops=2 * matmuls * rows * cols * depth, bytes_accessed=extra, transcendentals=rows * cols)


NEAR, FAR, OPPOSITE = -1, 1, 2
FOREIGN = [(NEAR, 0), (FAR, 0), (NEAR, 1), (FAR, 1), (FAR, 2), (NEAR, 2), (OPPOSITE, 0), (FAR, 3), (NEAR, 3), (OPPOSITE, 1), (OPPOSITE, 2), (OPPOSITE, 3)]
LINK = {item: item[1] for item in FOREIGN if item[0] == NEAR}
LINK.update({(FAR, 0): 4, (FAR, 1): 5, (OPPOSITE, 0): 6, (OPPOSITE, 1): 7, (FAR, 2): 8, (FAR, 3): 9, (OPPOSITE, 2): 10, (OPPOSITE, 3): 11})
SIBLING = 12
COPIES = SIBLING + PIECES + len(FOREIGN)
CHIPS = 4


def step_order():
    order = [(0, core, n) for core in (0, 1) for n in range(PIECES)]
    for a in range(0, len(FOREIGN), 2):
        pair = FOREIGN[a:a + 2]
        cores = [(0, pair[0]), (0, pair[1]), (1, pair[0]), (1, pair[1])]
        if a + 2 == len(FOREIGN):
            cores = [cores[0], cores[2], cores[1], cores[3]]
        order += [(chip, core, n) for core, (chip, n) in cores]
    return order


ORDER = step_order()


def place(chip, core, n):
    odd = lax.rem(lax.axis_index('dp'), 2)
    me = lax.axis_index('tp')
    sign = 1 - 2 * odd
    shard = lax.rem(me // 2 + chip * sign + CHIPS, CHIPS) * 2 + lax.rem(lax.rem(me, 2) + core, 2)
    return shard, lax.rem(odd * (PIECES // 2) + n, PIECES)


def logits_body(rows, h_ref, gain_ref, bias_ref, own_ref, *refs):
    x_refs = refs[:TOKEN_CHUNKS]
    lse_ref, norms_ref, all_ref, z_ref, e_buf, z_buf, m_ref, s_ref, e_sem, o_sem, z_sem, send_sem, recv_sem = refs[TOKEN_CHUNKS:]
    i = pl.program_id(0)
    steps = len(ORDER)
    tile = e_buf.shape[1]
    shard_rows = own_ref.shape[0]
    slot = lax.rem(i, 2)
    dp, me = lax.axis_index('dp'), lax.axis_index('tp')
    odd = lax.rem(dp, 2)
    sign = 1 - 2 * odd
    chip, core = me // 2, lax.rem(me, 2)
    targets = {
        'ahead': (dp, lax.rem(chip + sign + CHIPS, CHIPS) * 2 + core),
        'back': (dp, lax.rem(chip - sign + CHIPS, CHIPS) * 2 + core),
        'sibling': (dp, chip * 2 + 1 - core),
        'across': (dp + sign, me),
    }

    def rows_of(entry):
        shard, piece = place(*entry)
        return pl.ds(pl.multiple_of(shard * shard_rows + piece * tile, tile), tile)

    def own_rows(n):
        return pl.ds(pl.multiple_of(place(0, 0, n)[1] * tile, tile), tile)

    def remote(to, number, entry, own=False):
        at = rows_of(entry)
        source = own_ref.at[own_rows(entry[2]), :] if own else all_ref.at[at, :]
        return pltpu.make_async_remote_copy(source, all_ref.at[at, :], send_sem.at[number], recv_sem.at[number], device_id=targets[to], device_id_type=pl.DeviceIdType.MESH)

    def arrived(number):
        remote('sibling', number, ORDER[0]).wait_recv()

    def load(step):
        entry = ORDER[step]
        source = own_ref.at[own_rows(entry[2]), :] if step < PIECES else all_ref.at[rows_of(entry), :]
        pltpu.make_async_copy(source, e_buf.at[step % 2], e_sem.at[step % 2]).start()

    def keep(step):
        return pltpu.make_async_copy(e_buf.at[step % 2], all_ref.at[rows_of(ORDER[step]), :], o_sem.at[step % 2])

    def receive(step):
        chip_of, core_of, n = ORDER[step]
        if chip_of == 0 and core_of == 0:
            return
        if chip_of == 0:
            arrived(SIBLING + n)
            return
        number = FOREIGN.index((chip_of, n))
        if core_of == 1:
            arrived(SIBLING + PIECES + number)
            return
        arrived(LINK[chip_of, n])
        entry = ORDER[step]
        remote('sibling', SIBLING + PIECES + number, entry).start()
        if n < 2:
            if chip_of == FAR:
                remote('back', LINK[OPPOSITE, n], entry).start()
            elif chip_of == NEAR:
                remote('across', LINK[FAR, n + 2], entry).start()
            else:
                remote('across', LINK[OPPOSITE, n + 2], entry).start()

    @pl.when(i == 0)
    def _():
        barrier = pltpu.get_barrier_semaphore()
        for to in targets.values():
            pl.semaphore_signal(barrier, inc=1, device_id=to, device_id_type=pl.DeviceIdType.MESH)
        pl.semaphore_wait(barrier, len(targets))
        for n in range(PIECES):
            remote('ahead', LINK[NEAR, n], (0, 0, n), own=True).start()
            if n < 2:
                remote('back', LINK[FAR, n], (0, 0, n), own=True).start()
            remote('sibling', SIBLING + n, (0, 0, n), own=True).start()
        load(0)

        for c, x_ref in enumerate(x_refs):
            @pl.loop(0, x_ref.shape[0] // rows)
            def _(a, c=c, x_ref=x_ref):
                h = h_ref[pl.ds(pl.multiple_of(c * x_ref.shape[0] + a * rows, rows), rows), :].astype(F32)
                centred = h - jnp.mean(h, axis=-1, keepdims=True)
                inv_std = lax.rsqrt(jnp.mean(centred * centred, axis=-1, keepdims=True) + LN_EPS)
                x_ref[pl.ds(pl.multiple_of(a * rows, rows), rows), :] = (centred * inv_std * gain_ref[...] + bias_ref[...]).astype(BF16)
        m_ref[...] = jnp.full_like(m_ref, -jnp.inf)
        s_ref[...] = jnp.zeros_like(s_ref)

    pltpu.make_async_copy(own_ref.at[pl.ds(0, tile), :], e_buf.at[slot], e_sem.at[slot]).wait()
    for step in range(steps):
        @pl.when(i == step)
        def _(step=step):
            if step < PIECES:
                keep(step).start()
            if 1 <= step <= PIECES:
                keep(step - 1).wait()
            if step + 1 < steps:
                receive(step + 1)
                load(step + 1)

    def written(step):
        return pltpu.make_async_copy(z_buf.at[lax.rem(step, 2)], z_ref.at[:, pl.ds(pl.multiple_of(step * tile, tile), tile)], z_sem.at[lax.rem(step, 2)])

    @pl.when(i >= 2)
    def _():
        written(i - 2).wait()

    held = x_refs[0].shape[0]
    for r in range(0, h_ref.shape[0], rows):
        part = slice(r, r + rows)
        z = lax.dot_general(x_refs[r // held][r % held:r % held + rows, :], e_buf[slot], (((1,), (1,)), ((), ())), preferred_element_type=F32)
        z_buf[slot, part, :] = z
        m_old = m_ref[part, :]
        m_new = m_old
        for g in range(0, tile, LANES):
            m_new = jnp.maximum(m_new, z[:, g:g + LANES])
        total = s_ref[part, :] * jnp.exp(m_old - m_new)
        for g in range(0, tile, LANES):
            total = total + jnp.exp(z[:, g:g + LANES] - m_new)
        m_ref[part, :] = m_new
        s_ref[part, :] = total
    written(i).start()

    @pl.when(i == steps - 1)
    def _():
        m = m_ref[...]
        top = jnp.max(m, axis=-1, keepdims=True)
        total = jnp.sum(s_ref[...] * jnp.exp(m - top), axis=-1, keepdims=True)
        lse = jnp.broadcast_to(top + jnp.log(total), lse_ref.shape)
        lse_ref[...] = lse
        norms_ref[...] = lse.T[:norms_ref.shape[0]]
        written(i - 1).wait()
        written(i).wait()
        for number in range(COPIES):
            remote('sibling', number, ORDER[0]).wait_send()


def logits_call(hidden, gain, bias, embed, vocab, copies, rows=256):
    tokens, dim = hidden.shape
    tile = embed.shape[0] // PIECES
    whole = lambda shape: pl.BlockSpec(shape, lambda i: (0, 0), pipeline_mode=pl.Buffered(1))
    fixed = lambda shape: pl.BlockSpec(shape, lambda i: (0, 0))
    hbm = pl.BlockSpec(memory_space=pl.ANY)
    return pl.pallas_call(
        functools.partial(logits_body, rows),
        grid=(len(ORDER),),
        in_specs=[whole((tokens, dim)), whole((1, dim)), whole((1, dim)), hbm],
        out_specs=[fixed((tokens // TOKEN_CHUNKS, dim))] * TOKEN_CHUNKS + [fixed((tokens, LANES)), fixed((copies, tokens)), hbm, hbm],
        out_shape=[jax.ShapeDtypeStruct((tokens // TOKEN_CHUNKS, dim), BF16)] * TOKEN_CHUNKS + [
            jax.ShapeDtypeStruct((tokens, LANES), F32),
            jax.ShapeDtypeStruct((copies, tokens), F32),
            jax.ShapeDtypeStruct((vocab, dim), BF16),
            jax.ShapeDtypeStruct((tokens, vocab), F32),
        ],
        scratch_shapes=[
            pltpu.VMEM((2, tile, dim), BF16),
            pltpu.VMEM((2, tokens, tile), F32),
            pltpu.VMEM((tokens, LANES), F32),
            pltpu.VMEM((tokens, LANES), F32),
            pltpu.SemaphoreType.DMA((2,)),
            pltpu.SemaphoreType.DMA((2,)),
            pltpu.SemaphoreType.DMA((2,)),
            pltpu.SemaphoreType.DMA((COPIES,)),
            pltpu.SemaphoreType.DMA((COPIES,)),
        ],
        compiler_params=pltpu.CompilerParams(vmem_limit_bytes=VMEM_LIMIT, dimension_semantics=('arbitrary',), collective_id=0, has_side_effects=True),
        cost_estimate=cost(1, tokens, vocab, dim, 4 * tokens * vocab),
        name='logits',
    )(hidden, gain.reshape(1, dim), bias.reshape(1, dim), embed)


def own_grad_body(rows, order_ref, z_ref, e_ref, h_ref, gain_ref, lse_ref, tgt_row, w_row, dh_ref, loss_ref, sums_ref, acc_ref, t_ref, tgt_ref, w_ref):
    i = pl.program_id(0)
    tokens, tile = z_ref.shape
    base = order_ref[i] * tile

    @pl.when(i == 0)
    def _():
        acc_ref[...] = jnp.zeros_like(acc_ref)
        t_ref[...] = jnp.zeros_like(t_ref)
        tgt_ref[...] = jnp.broadcast_to(tgt_row[...], (LANES, tokens)).T
        w_ref[...] = jnp.broadcast_to(w_row[...], (LANES, tokens)).T

    lane = lax.broadcasted_iota(jnp.int32, (rows, LANES), 1)
    for r in range(0, tokens, rows):
        part = slice(r, r + rows)
        lse, tgt, w = lse_ref[part, :], tgt_ref[part, :] - base, w_ref[part, :]
        picked = t_ref[part, :]
        pieces = []
        for g in range(0, tile, LANES):
            z = z_ref[part, g:g + LANES]
            hit = lane + g == tgt
            p = jnp.exp(z - lse)
            p = jnp.where(hit, p - 1.0, p) * w
            picked = picked + jnp.where(hit, z, 0.0)
            pieces.append(p.astype(BF16))
        t_ref[part, :] = picked
        acc_ref[part, :] += jnp.dot(jnp.concatenate(pieces, axis=1), e_ref[...], preferred_element_type=F32)

    @pl.when(i == pl.num_programs(0) - 1)
    def _():
        loss = lse_ref[...] - jnp.sum(t_ref[...], axis=-1, keepdims=True)
        loss = jnp.where(w_ref[...] > 0.0, loss, 0.0)
        loss_ref[...] = loss.T[:8]
        sums_ref[...] = jnp.zeros_like(sums_ref)
        sums_ref[2:3, 0:LANES] = jnp.sum(loss, axis=0, keepdims=True)

        @pl.loop(0, tokens // rows)
        def _(a):
            part = pl.ds(pl.multiple_of(a * rows, rows), rows)
            h = h_ref[part, :].astype(F32)
            centred = h - jnp.mean(h, axis=-1, keepdims=True)
            inv_std = lax.rsqrt(jnp.mean(centred * centred, axis=-1, keepdims=True) + LN_EPS)
            x_hat = centred * inv_std
            d = acc_ref[part, :]
            sums_ref[0:1, :] += jnp.sum(d * x_hat, axis=0, keepdims=True)
            sums_ref[1:2, :] += jnp.sum(d, axis=0, keepdims=True)
            g = d * gain_ref[...]
            centre_term = jnp.mean(g, axis=-1, keepdims=True)
            proj_term = jnp.mean(g * x_hat, axis=-1, keepdims=True)
            dh_ref[part, :] = (inv_std * (g - centre_term - x_hat * proj_term)).astype(BF16)


def own_grad_call(order, z, e, hidden, gain, lse, tgt, w, tile, copies, rows=256):
    tokens, vocab = z.shape
    dim = e.shape[1]
    once = lambda shape: pl.BlockSpec(shape, lambda i, order: (0, 0), pipeline_mode=pl.Buffered(1))
    fixed = lambda shape: pl.BlockSpec(shape, lambda i, order: (0, 0))
    return pl.pallas_call(
        functools.partial(own_grad_body, rows),
        grid_spec=pltpu.PrefetchScalarGridSpec(
            num_scalar_prefetch=1,
            grid=(vocab // tile,),
            in_specs=[
                pl.BlockSpec((tokens, tile), lambda i, order: (0, i)),
                pl.BlockSpec((tile, dim), lambda i, order: (order[i], 0)),
                once((tokens, dim)),
                once((1, dim)),
                once((tokens, LANES)),
                once((1, tokens)),
                once((1, tokens)),
            ],
            out_specs=[fixed((tokens, dim)), fixed((8, tokens)), fixed((copies, dim))],
            scratch_shapes=[
                pltpu.VMEM((tokens, dim), F32),
                pltpu.VMEM((tokens, LANES), F32),
                pltpu.VMEM((tokens, LANES), jnp.int32),
                pltpu.VMEM((tokens, LANES), F32),
            ],
        ),
        out_shape=[
            jax.ShapeDtypeStruct((tokens, dim), BF16),
            jax.ShapeDtypeStruct((8, tokens), F32),
            jax.ShapeDtypeStruct((copies, dim), F32),
        ],
        compiler_params=params(),
        cost_estimate=cost(1, tokens, vocab, dim, 4 * tokens * vocab),
        name='own_grad',
    )(order, z, e, hidden, gain.reshape(1, dim), lse, tgt, w)


def d_embed_body(rows, first_ref, count_ref, x_ref, e_ref, lse_ref, info_ref, *refs):
    o_ref = refs[-1]

    @pl.when(pl.program_id(0) == 0)
    def _():
        if len(refs) == 1:
            o_ref[...] = jnp.zeros_like(o_ref)
        else:
            pltpu.sync_copy(refs[0], o_ref)

    width = x_ref.shape[0]
    info = info_ref[0:1, :]
    lse, tgt, w = lse_ref[0:1, :], (info >> 1) - first_ref[0], (info & 1).astype(F32) / count_ref[0]
    row = lax.broadcasted_iota(jnp.int32, (rows, width), 0)
    for r in range(0, e_ref.shape[0], rows):
        z = lax.dot_general(e_ref[r:r + rows, :], x_ref[...], (((1,), (1,)), ((), ())), preferred_element_type=F32)
        p = jnp.exp(z - lse)
        p = jnp.where(row == tgt - r, p - 1.0, p) * w
        o_ref[r:r + rows, :] += jnp.dot(p.astype(BF16), x_ref[...], preferred_element_type=F32)


def d_embed_call(first, count, x, e, lse, info, before, chunk, tile, rows=256):
    tokens, dim = x.shape
    shard = e.shape[0]
    scalar = pl.BlockSpec(memory_space=pltpu.SMEM)
    stat = lambda v: pl.BlockSpec((v.shape[0] * tile // tokens, tile), lambda i: (i, chunk))
    in_specs = [scalar, scalar, pl.BlockSpec((tile, dim), lambda i: (i, 0)), pl.BlockSpec((shard, dim), lambda i: (0, 0)), stat(lse), stat(info)]
    operands = [first.reshape(1), count.reshape(1), x, e, lse, info]
    if before is not None:
        in_specs.append(pl.BlockSpec(memory_space=pl.ANY))
        operands.append(before)
    return pl.pallas_call(
        functools.partial(d_embed_body, rows),
        grid=(tokens // tile,),
        in_specs=in_specs,
        out_specs=pl.BlockSpec((shard, dim), lambda i: (0, 0)),
        out_shape=jax.ShapeDtypeStruct((shard, dim), F32),
        compiler_params=params(),
        cost_estimate=cost(2, tokens, shard, dim, 2 * tokens * dim + 8 * shard * dim),
        name='d_embed',
    )(*operands)


def solution(mesh):
    group = mesh.shape['tp']

    def whole(hidden, ln_gain, ln_bias, embed, targets, loss_mask):
        tokens, dim = hidden.shape
        shard = embed.shape[0]
        rank = lax.axis_index('tp')
        copies = lambda width: -(-MIN_GATHER // (4 * group * width))
        info = lax.all_gather(jnp.tile((targets * 2 + loss_mask).reshape(1, tokens), (copies(tokens), 1)), 'tp', tiled=True)
        count = jnp.sum((info.reshape(group, -1, tokens)[:, 0] & 1).astype(F32))

        outs = logits_call(hidden, ln_gain, ln_bias, embed, shard * group, copies(tokens))
        lse, norms, all_embed, z = outs[TOKEN_CHUNKS:]
        x_chunks = []
        for h in range(TOKEN_CHUNKS):
            x_chunks.append(lax.all_gather(outs[h], 'tp', tiled=True))
        norms = lax.all_gather(norms, 'tp', tiled=True)

        places = [place(*entry) for entry in ORDER]
        order = jnp.stack([shard_of * PIECES + n for shard_of, n in places])
        scale = loss_mask.astype(F32) / count
        extra = -(-copies(dim) // 8) * 8
        d_hidden, loss, sums = own_grad_call(order, z, all_embed, hidden, ln_gain, lse, targets.reshape(1, tokens), scale.reshape(1, tokens), shard // PIECES, extra)
        sums = jnp.sum(lax.all_gather(sums, 'tp', tiled=True).reshape(group, extra, dim)[:, :3], axis=0)
        mean_loss = jnp.sum(sums[2, :LANES]) / LANES / count

        d_embed = None
        for h in range(TOKEN_CHUNKS):
            d_embed = d_embed_call(rank * shard, count, x_chunks[h], embed, norms, info, d_embed, h, tokens // TOKEN_CHUNKS)
        return loss[0], mean_loss.reshape(1), d_hidden, d_embed, sums[0], sums[1]

    token_rows = P(('dp', 'tp'))
    token_mat = P(('dp', 'tp'), None)
    return jax.shard_map(whole, mesh=mesh, in_specs=(token_mat, P(), P(), P('tp', None), token_rows, token_rows), out_specs=(token_rows, P('dp'), token_mat, token_mat, P('dp'), P('dp')), check_vma=False)
```

```python
import functools

import jax
import jax.numpy as jnp
from jax import lax
from jax.experimental import pallas as pl
from jax.experimental.pallas import tpu as pltpu
from jax.sharding import PartitionSpec as P


LN_EPS = 1e-5
F32 = jnp.float32
BF16 = jnp.bfloat16
LANES = 128
VMEM_LIMIT = 62 << 20
PIECES = 4
TOKEN_CHUNKS = 2
MIN_GATHER = 1 << 20


def params():
    return pltpu.CompilerParams(vmem_limit_bytes=VMEM_LIMIT, dimension_semantics=('arbitrary',))


def cost(matmuls, rows, cols, depth, extra):
    return pl.CostEstimate(flops=2 * matmuls * rows * cols * depth, bytes_accessed=extra, transcendentals=rows * cols)


NEAR, FAR, OPPOSITE = -1, 1, 2
FOREIGN = [(NEAR, 0), (FAR, 0), (NEAR, 1), (FAR, 1), (FAR, 2), (NEAR, 2), (OPPOSITE, 0), (FAR, 3), (NEAR, 3), (OPPOSITE, 1), (OPPOSITE, 2), (OPPOSITE, 3)]
LINK = {item: item[1] for item in FOREIGN if item[0] == NEAR}
LINK.update({(FAR, 0): 4, (FAR, 1): 5, (OPPOSITE, 0): 6, (OPPOSITE, 1): 7, (FAR, 2): 8, (FAR, 3): 9, (OPPOSITE, 2): 10, (OPPOSITE, 3): 11})
SPLIT = {'ahead': 12, 'back': 13, 'across': LINK[OPPOSITE, 3]}
SIBLING = 14
COPIES = SIBLING + PIECES + len(FOREIGN)
CHIPS = 4


def step_order():
    order = [(0, core, n) for core in (0, 1) for n in range(PIECES)]
    for a in range(0, len(FOREIGN), 2):
        pair = FOREIGN[a:a + 2]
        cores = [(0, pair[0]), (0, pair[1]), (1, pair[0]), (1, pair[1])]
        if a + 2 == len(FOREIGN):
            cores = [cores[0], cores[2], cores[1], cores[3]]
        order += [(chip, core, n) for core, (chip, n) in cores]
    return order


ORDER = step_order()


def place(chip, core, n):
    odd = lax.rem(lax.axis_index('dp'), 2)
    me = lax.axis_index('tp')
    sign = 1 - 2 * odd
    shard = lax.rem(me // 2 + chip * sign + CHIPS, CHIPS) * 2 + lax.rem(lax.rem(me, 2) + core, 2)
    return shard, lax.rem(odd * (PIECES // 2) + n, PIECES)


def logits_body(rows, h_ref, gain_ref, bias_ref, own_ref, *refs):
    x_refs = refs[:TOKEN_CHUNKS]
    lse_ref, norms_ref, all_ref, z_ref, zt_ref, e_buf, z_buf, t_buf, m_ref, s_ref, e_sem, o_sem, z_sem, t_sem, send_sem, recv_sem = refs[TOKEN_CHUNKS:]
    i = pl.program_id(0)
    steps = len(ORDER)
    tile = e_buf.shape[1]
    shard_rows = own_ref.shape[0]
    slot = lax.rem(i, 2)
    dp, me = lax.axis_index('dp'), lax.axis_index('tp')
    odd = lax.rem(dp, 2)
    sign = 1 - 2 * odd
    chip, core = me // 2, lax.rem(me, 2)
    targets = {
        'ahead': (dp, lax.rem(chip + sign + CHIPS, CHIPS) * 2 + core),
        'back': (dp, lax.rem(chip - sign + CHIPS, CHIPS) * 2 + core),
        'sibling': (dp, chip * 2 + 1 - core),
        'across': (dp + sign, me),
    }

    third = tile // 3 // 16 * 16 + 16
    shares = {'ahead': (0, third), 'back': (third, third), 'across': (2 * third, tile - 2 * third)}

    def rows_of(entry, share=None):
        shard, piece = place(*entry)
        begin, size = shares[share] if share else (0, tile)
        return pl.ds(pl.multiple_of(shard * shard_rows + piece * tile + begin, 16), size)

    def own_rows(n):
        return pl.ds(pl.multiple_of(place(0, 0, n)[1] * tile, tile), tile)

    def remote(to, number, entry, own=False, share=None):
        at = rows_of(entry, share)
        source = own_ref.at[own_rows(entry[2]), :] if own else all_ref.at[at, :]
        return pltpu.make_async_remote_copy(source, all_ref.at[at, :], send_sem.at[number], recv_sem.at[number], device_id=targets[to], device_id_type=pl.DeviceIdType.MESH)

    numbers = [(number, None) for number in range(COPIES) if number not in SPLIT.values()] + [(SPLIT[share], share) for share in SPLIT]

    def arrived(number, share=None):
        remote('sibling', number, ORDER[0], share=share).wait_recv()

    def load(step):
        entry = ORDER[step]
        source = own_ref.at[own_rows(entry[2]), :] if step < PIECES else all_ref.at[rows_of(entry), :]
        pltpu.make_async_copy(source, e_buf.at[step % 2], e_sem.at[step % 2]).start()

    def keep(step):
        return pltpu.make_async_copy(e_buf.at[step % 2], all_ref.at[rows_of(ORDER[step]), :], o_sem.at[step % 2])

    def receive(step):
        chip_of, core_of, n = ORDER[step]
        if chip_of == 0 and core_of == 0:
            return
        if chip_of == 0:
            arrived(SIBLING + n)
            return
        number = FOREIGN.index((chip_of, n))
        if core_of == 1:
            arrived(SIBLING + PIECES + number)
            return
        if (chip_of, n) == (OPPOSITE, 3):
            for share in SPLIT:
                arrived(SPLIT[share], share)
        else:
            arrived(LINK[chip_of, n])
        entry = ORDER[step]
        remote('sibling', SIBLING + PIECES + number, entry).start()
        if n < 2:
            if chip_of == FAR:
                remote('back', LINK[OPPOSITE, n], entry).start()
            elif chip_of == NEAR:
                remote('across', LINK[FAR, n + 2], entry).start()
            else:
                share = 'across' if n == 1 else None
                remote('across', LINK[OPPOSITE, n + 2], entry, share=share).start()
        elif n == 3 and chip_of != OPPOSITE:
            share = 'ahead' if chip_of == NEAR else 'back'
            remote(share, SPLIT[share], entry, share=share).start()

    @pl.when(i == 0)
    def _():
        barrier = pltpu.get_barrier_semaphore()
        for to in targets.values():
            pl.semaphore_signal(barrier, inc=1, device_id=to, device_id_type=pl.DeviceIdType.MESH)
        pl.semaphore_wait(barrier, len(targets))
        for n in range(PIECES):
            remote('ahead', LINK[NEAR, n], (0, 0, n), own=True).start()
            if n < 2:
                remote('back', LINK[FAR, n], (0, 0, n), own=True).start()
            remote('sibling', SIBLING + n, (0, 0, n), own=True).start()
        load(0)

        for c, x_ref in enumerate(x_refs):
            @pl.loop(0, x_ref.shape[0] // rows)
            def _(a, c=c, x_ref=x_ref):
                h = h_ref[pl.ds(pl.multiple_of(c * x_ref.shape[0] + a * rows, rows), rows), :].astype(F32)
                centred = h - jnp.mean(h, axis=-1, keepdims=True)
                inv_std = lax.rsqrt(jnp.mean(centred * centred, axis=-1, keepdims=True) + LN_EPS)
                x_ref[pl.ds(pl.multiple_of(a * rows, rows), rows), :] = (centred * inv_std * gain_ref[...] + bias_ref[...]).astype(BF16)
        m_ref[...] = jnp.full_like(m_ref, -jnp.inf)
        s_ref[...] = jnp.zeros_like(s_ref)

    pltpu.make_async_copy(own_ref.at[pl.ds(0, tile), :], e_buf.at[slot], e_sem.at[slot]).wait()
    for step in range(steps):
        @pl.when(i == step)
        def _(step=step):
            if step < PIECES:
                keep(step).start()
            if 1 <= step <= PIECES:
                keep(step - 1).wait()
            if step + 1 < steps:
                receive(step + 1)
                load(step + 1)

    def written(step):
        return pltpu.make_async_copy(z_buf.at[lax.rem(step, 2)], z_ref.at[:, pl.ds(pl.multiple_of(step * tile, tile), tile)], z_sem.at[lax.rem(step, 2)])

    @pl.when(i >= 2)
    def _():
        written(i - 2).wait()

    held = x_refs[0].shape[0]
    for r in range(0, h_ref.shape[0], rows):
        part = slice(r, r + rows)
        z = lax.dot_general(x_refs[r // held][r % held:r % held + rows, :], e_buf[slot], (((1,), (1,)), ((), ())), preferred_element_type=F32)
        z_buf[slot, part, :] = z
        m_old = m_ref[part, :]
        m_new = m_old
        for g in range(0, tile, LANES):
            m_new = jnp.maximum(m_new, z[:, g:g + LANES])
        total = s_ref[part, :] * jnp.exp(m_old - m_new)
        for g in range(0, tile, LANES):
            total = total + jnp.exp(z[:, g:g + LANES] - m_new)
        m_ref[part, :] = m_new
        s_ref[part, :] = total
    written(i).start()

    def turned(step):
        return pltpu.make_async_copy(t_buf, zt_ref.at[own_rows(step), :], t_sem)

    @pl.when((i >= 1) & (i <= PIECES))
    def _():
        turned(i - 1).wait()

    @pl.when(i < PIECES)
    def _():
        for r in range(0, h_ref.shape[0], rows):
            t_buf[:, r:r + rows] = lax.dot_general(e_buf[slot], x_refs[r // held][r % held:r % held + rows, :], (((1,), (1,)), ((), ())), preferred_element_type=F32)
        turned(i).start()

    @pl.when(i == steps - 1)
    def _():
        m = m_ref[...]
        top = jnp.max(m, axis=-1, keepdims=True)
        total = jnp.sum(s_ref[...] * jnp.exp(m - top), axis=-1, keepdims=True)
        lse = jnp.broadcast_to(top + jnp.log(total), lse_ref.shape)
        lse_ref[...] = lse
        norms_ref[...] = lse.T[:norms_ref.shape[0]]
        written(i - 1).wait()
        written(i).wait()
        for number, share in numbers:
            remote('sibling', number, ORDER[0], share=share).wait_send()


def logits_call(hidden, gain, bias, embed, vocab, copies, rows=256):
    tokens, dim = hidden.shape
    tile = embed.shape[0] // PIECES
    whole = lambda shape: pl.BlockSpec(shape, lambda i: (0, 0), pipeline_mode=pl.Buffered(1))
    fixed = lambda shape: pl.BlockSpec(shape, lambda i: (0, 0))
    hbm = pl.BlockSpec(memory_space=pl.ANY)
    line = pl.BlockSpec((dim,), lambda i: (0,))
    return pl.pallas_call(
        functools.partial(logits_body, rows),
        grid=(len(ORDER),),
        in_specs=[whole((tokens, dim)), line, line, hbm],
        out_specs=[fixed((tokens // TOKEN_CHUNKS, dim))] * TOKEN_CHUNKS + [fixed((tokens, LANES)), fixed((copies, tokens)), hbm, hbm, hbm],
        out_shape=[jax.ShapeDtypeStruct((tokens // TOKEN_CHUNKS, dim), BF16)] * TOKEN_CHUNKS + [
            jax.ShapeDtypeStruct((tokens, LANES), F32),
            jax.ShapeDtypeStruct((copies, tokens), F32),
            jax.ShapeDtypeStruct((vocab, dim), BF16),
            jax.ShapeDtypeStruct((tokens, vocab), F32),
            jax.ShapeDtypeStruct((embed.shape[0], tokens), F32),
        ],
        scratch_shapes=[
            pltpu.VMEM((2, tile, dim), BF16),
            pltpu.VMEM((2, tokens, tile), F32),
            pltpu.VMEM((tile, tokens), F32),
            pltpu.VMEM((tokens, LANES), F32),
            pltpu.VMEM((tokens, LANES), F32),
            pltpu.SemaphoreType.DMA((2,)),
            pltpu.SemaphoreType.DMA((2,)),
            pltpu.SemaphoreType.DMA((2,)),
            pltpu.SemaphoreType.DMA,
            pltpu.SemaphoreType.DMA((COPIES,)),
            pltpu.SemaphoreType.DMA((COPIES,)),
        ],
        compiler_params=pltpu.CompilerParams(vmem_limit_bytes=VMEM_LIMIT, dimension_semantics=('arbitrary',), collective_id=0, has_side_effects=True),
        cost_estimate=cost(1, tokens, vocab, dim, 4 * tokens * vocab),
        name='logits',
    )(hidden, gain, bias, embed)


def own_grad_body(rows, repeats, order_ref, z_ref, e_ref, h_ref, gain_ref, lse_ref, info_ref, dh_ref, loss_ref, sums_ref, count_ref, acc_ref, t_ref, tgt_ref, w_ref):
    i = pl.program_id(0)
    tokens, tile = z_ref.shape
    base = order_ref[i] * tile

    @pl.when(i == 0)
    def _():
        acc_ref[...] = jnp.zeros_like(acc_ref)
        t_ref[...] = jnp.zeros_like(t_ref)
        total = jnp.sum((info_ref[...] & 1).astype(F32)) / repeats
        count_ref[...] = jnp.full_like(count_ref, total)
        own = info_ref[pl.ds(pl.multiple_of(lax.axis_index('tp') * repeats, repeats), 1), :]
        tgt_ref[...] = jnp.broadcast_to(own >> 1, (LANES, tokens)).T
        w_ref[...] = jnp.broadcast_to((own & 1).astype(F32) / count_ref[0:1, 0:1], (LANES, tokens)).T

    lane = lax.broadcasted_iota(jnp.int32, (rows, LANES), 1)
    for r in range(0, tokens, rows):
        part = slice(r, r + rows)
        lse, tgt, w = lse_ref[part, :], tgt_ref[part, :] - base, w_ref[part, :]
        picked = t_ref[part, :]
        pieces = []
        for g in range(0, tile, LANES):
            z = z_ref[part, g:g + LANES]
            hit = lane + g == tgt
            p = jnp.exp(z - lse)
            p = jnp.where(hit, p - 1.0, p) * w
            picked = picked + jnp.where(hit, z, 0.0)
            pieces.append(p.astype(BF16))
        t_ref[part, :] = picked
        acc_ref[part, :] += jnp.dot(jnp.concatenate(pieces, axis=1), e_ref[...], preferred_element_type=F32)

    @pl.when(i == pl.num_programs(0) - 1)
    def _():
        loss = lse_ref[...] - jnp.sum(t_ref[...], axis=-1, keepdims=True)
        loss = jnp.where(w_ref[...] > 0.0, loss, 0.0)
        loss_ref[...] = loss.T[:8]
        sums_ref[...] = jnp.zeros_like(sums_ref)
        sums_ref[2:3, 0:LANES] = jnp.sum(loss, axis=0, keepdims=True)

        @pl.loop(0, tokens // rows)
        def _(a):
            part = pl.ds(pl.multiple_of(a * rows, rows), rows)
            h = h_ref[part, :].astype(F32)
            centred = h - jnp.mean(h, axis=-1, keepdims=True)
            inv_std = lax.rsqrt(jnp.mean(centred * centred, axis=-1, keepdims=True) + LN_EPS)
            x_hat = centred * inv_std
            d = acc_ref[part, :]
            sums_ref[0:1, :] += jnp.sum(d * x_hat, axis=0, keepdims=True)
            sums_ref[1:2, :] += jnp.sum(d, axis=0, keepdims=True)
            g = d * gain_ref[...]
            centre_term = jnp.mean(g, axis=-1, keepdims=True)
            proj_term = jnp.mean(g * x_hat, axis=-1, keepdims=True)
            dh_ref[part, :] = (inv_std * (g - centre_term - x_hat * proj_term)).astype(BF16)


def own_grad_call(order, z, e, hidden, gain, lse, info, tile, copies, rows=256):
    tokens, vocab = z.shape
    dim = e.shape[1]
    once = lambda shape: pl.BlockSpec(shape, lambda i, order: (0, 0), pipeline_mode=pl.Buffered(1))
    fixed = lambda shape: pl.BlockSpec(shape, lambda i, order: (0, 0))
    return pl.pallas_call(
        functools.partial(own_grad_body, rows, info.shape[0] * tokens // vocab),
        grid_spec=pltpu.PrefetchScalarGridSpec(
            num_scalar_prefetch=1,
            grid=(vocab // tile,),
            in_specs=[
                pl.BlockSpec((tokens, tile), lambda i, order: (0, i)),
                pl.BlockSpec((tile, dim), lambda i, order: (order[i], 0)),
                once((tokens, dim)),
                pl.BlockSpec((dim,), lambda i, order: (0,)),
                once((tokens, LANES)),
                once(info.shape),
            ],
            out_specs=[fixed((tokens, dim)), fixed((8, tokens)), fixed((copies, dim)), fixed((8, LANES))],
            scratch_shapes=[
                pltpu.VMEM((tokens, dim), F32),
                pltpu.VMEM((tokens, LANES), F32),
                pltpu.VMEM((tokens, LANES), jnp.int32),
                pltpu.VMEM((tokens, LANES), F32),
            ],
        ),
        out_shape=[
            jax.ShapeDtypeStruct((tokens, dim), BF16),
            jax.ShapeDtypeStruct((8, tokens), F32),
            jax.ShapeDtypeStruct((copies, dim), F32),
            jax.ShapeDtypeStruct((8, LANES), F32),
        ],
        compiler_params=params(),
        cost_estimate=cost(1, tokens, vocab, dim, 4 * tokens * vocab),
        name='own_grad',
    )(order, z, e, hidden, gain, lse, info)


def d_embed_body(rows, chunk, rank_ref, x_ref, e_ref, lse_ref, info_ref, count_ref, zt_ref, *refs):
    o_ref, z_buf, z_sem = refs[-3:] if len(refs) == 3 else refs[1:4]
    i = pl.program_id(0)
    last = pl.num_programs(0) - 1
    shard, width = e_ref.shape[0], x_ref.shape[0]
    fetches = [pltpu.make_async_copy(zt_ref.at[:, chunk * width:(chunk + 1) * width], z_buf, z_sem)]
    if len(refs) > 3:
        before_ref, before_buf, before_sem = refs[0], refs[4], refs[5]
        fetches.append(pltpu.make_async_copy(before_ref, before_buf, before_sem))

    @pl.when(i == 0)
    def _():
        for fetch in fetches:
            fetch.start()
        o_ref[...] = jnp.zeros_like(o_ref)

    info = info_ref[0:1, :]
    lse, tgt, w = lse_ref[0:1, :], (info >> 1) - rank_ref[0] * shard, (info & 1).astype(F32) / count_ref[0:1, 0:1]

    def part_of(r, z):
        row = lax.broadcasted_iota(jnp.int32, (rows, width), 0)
        p = jnp.exp(z - lse)
        p = jnp.where(row == tgt - r, p - 1.0, p) * w
        return jnp.dot(p.astype(BF16), x_ref[...], preferred_element_type=F32)

    @pl.when(i < last)
    def _():
        for r in range(0, shard, rows):
            z = lax.dot_general(e_ref[r:r + rows, :], x_ref[...], (((1,), (1,)), ((), ())), preferred_element_type=F32)
            o_ref[r:r + rows, :] += part_of(r, z)

    @pl.when(i == last)
    def _():
        for fetch in fetches:
            fetch.wait()
        for r in range(0, shard, rows):
            total = o_ref[r:r + rows, :] + part_of(r, z_buf[r:r + rows, :])
            if len(fetches) > 1:
                total = total + before_buf[r:r + rows, :]
            o_ref[r:r + rows, :] = total


def d_embed_call(rank, count, x, e, lse, info, zt, before, chunk, tile, rows=256):
    tokens, dim = x.shape
    shard = e.shape[0]
    group = tokens // tile
    whose = lambda i, rank: lax.rem(rank[0] + 1 + i, group)
    stat = lambda v: pl.BlockSpec((v.shape[0] // group, tile), lambda i, rank: (whose(i, rank), chunk))
    once = lambda shape: pl.BlockSpec(shape, lambda i, rank: (0, 0), pipeline_mode=pl.Buffered(1))
    hbm = pl.BlockSpec(memory_space=pl.ANY)
    in_specs = [pl.BlockSpec((tile, dim), lambda i, rank: (whose(i, rank), 0)), once((shard, dim)), stat(lse), stat(info), once(count.shape), hbm]
    operands = [x, e, lse, info, count, zt]
    scratch = [pltpu.VMEM((shard, tile), F32), pltpu.SemaphoreType.DMA]
    if before is not None:
        in_specs.append(hbm)
        operands.append(before)
        scratch += [pltpu.VMEM((shard, dim), F32), pltpu.SemaphoreType.DMA]
    return pl.pallas_call(
        functools.partial(d_embed_body, rows, chunk),
        grid_spec=pltpu.PrefetchScalarGridSpec(
            num_scalar_prefetch=1,
            grid=(group,),
            in_specs=in_specs,
            out_specs=pl.BlockSpec((shard, dim), lambda i, rank: (0, 0)),
            scratch_shapes=scratch,
        ),
        out_shape=jax.ShapeDtypeStruct((shard, dim), F32),
        compiler_params=params(),
        cost_estimate=cost(2, tokens, shard, dim, 2 * tokens * dim + 8 * shard * dim),
        name='d_embed',
    )(rank.reshape(1), *operands)


def solution(mesh):
    group = mesh.shape['tp']

    def whole(hidden, ln_gain, ln_bias, embed, targets, loss_mask):
        tokens, dim = hidden.shape
        shard = embed.shape[0]
        rank = lax.axis_index('tp')
        copies = lambda width: -(-MIN_GATHER // (4 * group * width))
        info = lax.all_gather(jnp.tile((targets * 2 + loss_mask).reshape(1, tokens), (copies(tokens), 1)), 'tp', tiled=True)

        outs = logits_call(hidden, ln_gain, ln_bias, embed, shard * group, copies(tokens))
        lse, norms, all_embed, z, zt = outs[TOKEN_CHUNKS:]
        x_chunks = []
        for h in range(TOKEN_CHUNKS):
            x_chunks.append(lax.all_gather(outs[h], 'tp', tiled=True))
        norms = lax.all_gather(norms, 'tp', tiled=True)

        places = [place(*entry) for entry in ORDER]
        order = jnp.stack([shard_of * PIECES + n for shard_of, n in places])
        extra = -(-copies(dim) // 8) * 8
        d_hidden, loss, sums, count = own_grad_call(order, z, all_embed, hidden, ln_gain, lse, info, shard // PIECES, extra)
        sums = jnp.sum(lax.all_gather(sums, 'tp', tiled=True).reshape(group, extra, dim)[:, :3], axis=0)
        mean_loss = sums[2, 0] / count[0, 0]

        d_embed = None
        for h in range(TOKEN_CHUNKS):
            d_embed = d_embed_call(rank, count, x_chunks[h], embed, norms, info, zt, d_embed, h, tokens // TOKEN_CHUNKS)
        return loss[0], mean_loss.reshape(1), d_hidden, d_embed, sums[0], sums[1]

    token_rows = P(('dp', 'tp'))
    token_mat = P(('dp', 'tp'), None)
    return jax.shard_map(whole, mesh=mesh, in_specs=(token_mat, P(), P(), P('tp', None), token_rows, token_rows), out_specs=(token_rows, P('dp'), token_mat, token_mat, P('dp'), P('dp')), check_vma=False)
```

```python
import functools

import jax
import jax.numpy as jnp
from jax import lax
from jax.experimental import pallas as pl
from jax.experimental.pallas import tpu as pltpu
from jax.sharding import PartitionSpec as P


LN_EPS = 1e-5
F32 = jnp.float32
BF16 = jnp.bfloat16
LANES = 128
VMEM_LIMIT = 62 << 20
PIECES = 4
TOKEN_CHUNKS = 2
MIN_GATHER = 1 << 20


def params():
    return pltpu.CompilerParams(vmem_limit_bytes=VMEM_LIMIT, dimension_semantics=('arbitrary',))


def cost(matmuls, rows, cols, depth, extra):
    return pl.CostEstimate(flops=2 * matmuls * rows * cols * depth, bytes_accessed=extra, transcendentals=rows * cols)


NEAR, FAR, OPPOSITE = -1, 1, 2
FOREIGN = [(NEAR, 0), (FAR, 0), (NEAR, 1), (FAR, 1), (FAR, 2), (NEAR, 2), (OPPOSITE, 0), (FAR, 3), (NEAR, 3), (OPPOSITE, 1), (OPPOSITE, 2), (OPPOSITE, 3)]
LINK = {item: item[1] for item in FOREIGN if item[0] == NEAR}
LINK.update({(FAR, 0): 4, (FAR, 1): 5, (OPPOSITE, 0): 6, (OPPOSITE, 1): 7, (FAR, 2): 8, (FAR, 3): 9, (OPPOSITE, 2): 10, (OPPOSITE, 3): 11})
SPLIT = {'ahead': 12, 'back': 13, 'across': LINK[OPPOSITE, 3]}
SIBLING = 14
COPIES = SIBLING + PIECES + len(FOREIGN)
CHIPS = 4


def step_order():
    order = [(0, core, n) for core in (0, 1) for n in range(PIECES)]
    for a in range(0, len(FOREIGN), 2):
        pair = FOREIGN[a:a + 2]
        cores = [(0, pair[0]), (0, pair[1]), (1, pair[0]), (1, pair[1])]
        if a + 2 == len(FOREIGN):
            cores = [cores[0], cores[2], cores[1], cores[3]]
        order += [(chip, core, n) for core, (chip, n) in cores]
    return order


ORDER = step_order()


def place(chip, core, n):
    odd = lax.rem(lax.axis_index('dp'), 2)
    me = lax.axis_index('tp')
    sign = 1 - 2 * odd
    shard = lax.rem(me // 2 + chip * sign + CHIPS, CHIPS) * 2 + lax.rem(lax.rem(me, 2) + core, 2)
    return shard, lax.rem(odd * (PIECES // 2) + n, PIECES)


def logits_body(rows, h_ref, gain_ref, bias_ref, own_ref, *refs):
    x_refs = refs[:TOKEN_CHUNKS]
    lse_ref, norms_ref, all_ref, z_ref, zt_ref, e_buf, z_buf, t_buf, m_ref, s_ref, e_sem, o_sem, z_sem, t_sem, send_sem, recv_sem = refs[TOKEN_CHUNKS:]
    i = pl.program_id(0)
    steps = len(ORDER)
    tile = e_buf.shape[1]
    shard_rows = own_ref.shape[0]
    slot = lax.rem(i, 2)
    dp, me = lax.axis_index('dp'), lax.axis_index('tp')
    odd = lax.rem(dp, 2)
    sign = 1 - 2 * odd
    chip, core = me // 2, lax.rem(me, 2)
    targets = {
        'ahead': (dp, lax.rem(chip + sign + CHIPS, CHIPS) * 2 + core),
        'back': (dp, lax.rem(chip - sign + CHIPS, CHIPS) * 2 + core),
        'sibling': (dp, chip * 2 + 1 - core),
        'across': (dp + sign, me),
    }

    third = tile // 3 // 16 * 16 + 16
    shares = {'ahead': (0, third), 'back': (third, third), 'across': (2 * third, tile - 2 * third)}

    def rows_of(entry, share=None):
        shard, piece = place(*entry)
        begin, size = shares[share] if share else (0, tile)
        return pl.ds(pl.multiple_of(shard * shard_rows + piece * tile + begin, 16), size)

    def own_rows(n):
        return pl.ds(pl.multiple_of(place(0, 0, n)[1] * tile, tile), tile)

    def remote(to, number, entry, own=False, share=None):
        at = rows_of(entry, share)
        source = own_ref.at[own_rows(entry[2]), :] if own else all_ref.at[at, :]
        return pltpu.make_async_remote_copy(source, all_ref.at[at, :], send_sem.at[number], recv_sem.at[number], device_id=targets[to], device_id_type=pl.DeviceIdType.MESH)

    numbers = [(number, None) for number in range(COPIES) if number not in SPLIT.values()] + [(SPLIT[share], share) for share in SPLIT]

    def arrived(number, share=None):
        remote('sibling', number, ORDER[0], share=share).wait_recv()

    def load(step):
        entry = ORDER[step]
        source = own_ref.at[own_rows(entry[2]), :] if step < PIECES else all_ref.at[rows_of(entry), :]
        pltpu.make_async_copy(source, e_buf.at[step % 2], e_sem.at[step % 2]).start()

    def keep(step):
        return pltpu.make_async_copy(e_buf.at[step % 2], all_ref.at[rows_of(ORDER[step]), :], o_sem.at[step % 2])

    def receive(step):
        chip_of, core_of, n = ORDER[step]
        if chip_of == 0 and core_of == 0:
            return
        if chip_of == 0:
            arrived(SIBLING + n)
            return
        number = FOREIGN.index((chip_of, n))
        if core_of == 1:
            arrived(SIBLING + PIECES + number)
            return
        if (chip_of, n) == (OPPOSITE, 3):
            for share in SPLIT:
                arrived(SPLIT[share], share)
        else:
            arrived(LINK[chip_of, n])
        entry = ORDER[step]
        remote('sibling', SIBLING + PIECES + number, entry).start()
        if n < 2:
            if chip_of == FAR:
                remote('back', LINK[OPPOSITE, n], entry).start()
            elif chip_of == NEAR:
                remote('across', LINK[FAR, n + 2], entry).start()
            else:
                share = 'across' if n == 1 else None
                remote('across', LINK[OPPOSITE, n + 2], entry, share=share).start()
        elif n == 3 and chip_of != OPPOSITE:
            share = 'ahead' if chip_of == NEAR else 'back'
            remote(share, SPLIT[share], entry, share=share).start()

    @pl.when(i == 0)
    def _():
        barrier = pltpu.get_barrier_semaphore()
        for to in targets.values():
            pl.semaphore_signal(barrier, inc=1, device_id=to, device_id_type=pl.DeviceIdType.MESH)
        pl.semaphore_wait(barrier, len(targets))
        for n in range(PIECES):
            remote('ahead', LINK[NEAR, n], (0, 0, n), own=True).start()
            if n < 2:
                remote('back', LINK[FAR, n], (0, 0, n), own=True).start()
            remote('sibling', SIBLING + n, (0, 0, n), own=True).start()
        load(0)

        for c, x_ref in enumerate(x_refs):
            @pl.loop(0, x_ref.shape[0] // rows)
            def _(a, c=c, x_ref=x_ref):
                h = h_ref[pl.ds(pl.multiple_of(c * x_ref.shape[0] + a * rows, rows), rows), :].astype(F32)
                centred = h - jnp.mean(h, axis=-1, keepdims=True)
                inv_std = lax.rsqrt(jnp.mean(centred * centred, axis=-1, keepdims=True) + LN_EPS)
                x_ref[pl.ds(pl.multiple_of(a * rows, rows), rows), :] = (centred * inv_std * gain_ref[...] + bias_ref[...]).astype(BF16)
        m_ref[...] = jnp.full_like(m_ref, -jnp.inf)
        s_ref[...] = jnp.zeros_like(s_ref)

    pltpu.make_async_copy(own_ref.at[pl.ds(0, tile), :], e_buf.at[slot], e_sem.at[slot]).wait()
    for step in range(steps):
        @pl.when(i == step)
        def _(step=step):
            if step < PIECES:
                keep(step).start()
            if 1 <= step <= PIECES:
                keep(step - 1).wait()
            if step + 1 < steps:
                receive(step + 1)
                load(step + 1)

    def written(step):
        return pltpu.make_async_copy(z_buf.at[lax.rem(step, 2)], z_ref.at[:, pl.ds(pl.multiple_of(step * tile, tile), tile)], z_sem.at[lax.rem(step, 2)])

    @pl.when(i >= 2)
    def _():
        written(i - 2).wait()

    held = x_refs[0].shape[0]
    for c, x_ref in enumerate(x_refs):
        @pl.loop(0, held // (2 * rows))
        def _(a, c=c, x_ref=x_ref):
            for b in range(2):
                from_ = pl.multiple_of((2 * a + b) * rows, rows)
                part = pl.ds(pl.multiple_of(c * held + from_, rows), rows)
                z = lax.dot_general(x_ref[pl.ds(from_, rows), :], e_buf[slot], (((1,), (1,)), ((), ())), preferred_element_type=F32)
                z_buf[slot, part, :] = z
                m_old = m_ref[part, :]
                m_new = m_old
                for g in range(0, tile, LANES):
                    m_new = jnp.maximum(m_new, z[:, g:g + LANES])
                total = s_ref[part, :] * jnp.exp(m_old - m_new)
                for g in range(0, tile, LANES):
                    total = total + jnp.exp(z[:, g:g + LANES] - m_new)
                m_ref[part, :] = m_new
                s_ref[part, :] = total
    written(i).start()

    def turned(step):
        return pltpu.make_async_copy(t_buf, zt_ref.at[own_rows(step), :], t_sem)

    @pl.when((i >= 1) & (i <= PIECES))
    def _():
        turned(i - 1).wait()

    @pl.when(i < PIECES)
    def _():
        for c, x_ref in enumerate(x_refs):
            @pl.loop(0, tile // LANES)
            def _(a, c=c, x_ref=x_ref):
                part = pl.ds(pl.multiple_of(a * LANES, LANES), LANES)
                t_buf[part, c * held:(c + 1) * held] = lax.dot_general(e_buf[slot, part, :], x_ref[...], (((1,), (1,)), ((), ())), preferred_element_type=F32)
        turned(i).start()

    @pl.when(i == steps - 1)
    def _():
        m = m_ref[...]
        top = jnp.max(m, axis=-1, keepdims=True)
        total = jnp.sum(s_ref[...] * jnp.exp(m - top), axis=-1, keepdims=True)
        lse = jnp.broadcast_to(top + jnp.log(total), lse_ref.shape)
        lse_ref[...] = lse
        norms_ref[...] = lse.T[:norms_ref.shape[0]]
        written(i - 1).wait()
        written(i).wait()
        for number, share in numbers:
            remote('sibling', number, ORDER[0], share=share).wait_send()


def logits_call(hidden, gain, bias, embed, vocab, copies, rows=256):
    tokens, dim = hidden.shape
    tile = embed.shape[0] // PIECES
    whole = lambda shape: pl.BlockSpec(shape, lambda i: (0, 0), pipeline_mode=pl.Buffered(1))
    fixed = lambda shape: pl.BlockSpec(shape, lambda i: (0, 0))
    hbm = pl.BlockSpec(memory_space=pl.ANY)
    line = pl.BlockSpec((dim,), lambda i: (0,))
    return pl.pallas_call(
        functools.partial(logits_body, rows),
        grid=(len(ORDER),),
        in_specs=[whole((tokens, dim)), line, line, hbm],
        out_specs=[fixed((tokens // TOKEN_CHUNKS, dim))] * TOKEN_CHUNKS + [fixed((tokens, LANES)), fixed((copies, tokens)), hbm, hbm, hbm],
        out_shape=[jax.ShapeDtypeStruct((tokens // TOKEN_CHUNKS, dim), BF16)] * TOKEN_CHUNKS + [
            jax.ShapeDtypeStruct((tokens, LANES), F32),
            jax.ShapeDtypeStruct((copies, tokens), F32),
            jax.ShapeDtypeStruct((vocab, dim), BF16),
            jax.ShapeDtypeStruct((tokens, vocab), F32),
            jax.ShapeDtypeStruct((embed.shape[0], tokens), F32),
        ],
        scratch_shapes=[
            pltpu.VMEM((2, tile, dim), BF16),
            pltpu.VMEM((2, tokens, tile), F32),
            pltpu.VMEM((tile, tokens), F32),
            pltpu.VMEM((tokens, LANES), F32),
            pltpu.VMEM((tokens, LANES), F32),
            pltpu.SemaphoreType.DMA((2,)),
            pltpu.SemaphoreType.DMA((2,)),
            pltpu.SemaphoreType.DMA((2,)),
            pltpu.SemaphoreType.DMA,
            pltpu.SemaphoreType.DMA((COPIES,)),
            pltpu.SemaphoreType.DMA((COPIES,)),
        ],
        compiler_params=pltpu.CompilerParams(vmem_limit_bytes=VMEM_LIMIT, dimension_semantics=('arbitrary',), collective_id=0, has_side_effects=True),
        cost_estimate=cost(1, tokens, vocab, dim, 4 * tokens * vocab),
        name='logits',
    )(hidden, gain, bias, embed)


def own_grad_body(rows, repeats, order_ref, z_ref, e_ref, h_ref, gain_ref, lse_ref, info_ref, dh_ref, loss_ref, sums_ref, count_ref, acc_ref, t_ref, tgt_ref, w_ref):
    i = pl.program_id(0)
    tokens, tile = z_ref.shape
    base = order_ref[i] * tile

    @pl.when(i == 0)
    def _():
        acc_ref[...] = jnp.zeros_like(acc_ref)
        t_ref[...] = jnp.zeros_like(t_ref)
        total = jnp.sum((info_ref[...] & 1).astype(F32)) / repeats
        count_ref[...] = jnp.full_like(count_ref, total)
        own = info_ref[pl.ds(pl.multiple_of(lax.axis_index('tp') * repeats, repeats), 1), :]
        tgt_ref[...] = jnp.broadcast_to(own >> 1, (LANES, tokens)).T
        w_ref[...] = jnp.broadcast_to((own & 1).astype(F32) / count_ref[0:1, 0:1], (LANES, tokens)).T

    lane = lax.broadcasted_iota(jnp.int32, (rows, LANES), 1)
    for r in range(0, tokens, rows):
        part = slice(r, r + rows)
        lse, tgt, w = lse_ref[part, :], tgt_ref[part, :] - base, w_ref[part, :]
        picked = t_ref[part, :]
        pieces = []
        for g in range(0, tile, LANES):
            z = z_ref[part, g:g + LANES]
            hit = lane + g == tgt
            p = jnp.exp(z - lse)
            p = jnp.where(hit, p - 1.0, p) * w
            picked = picked + jnp.where(hit, z, 0.0)
            pieces.append(p.astype(BF16))
        t_ref[part, :] = picked
        acc_ref[part, :] += jnp.dot(jnp.concatenate(pieces, axis=1), e_ref[...], preferred_element_type=F32)

    @pl.when(i == pl.num_programs(0) - 1)
    def _():
        loss = lse_ref[...] - jnp.sum(t_ref[...], axis=-1, keepdims=True)
        loss = jnp.where(w_ref[...] > 0.0, loss, 0.0)
        loss_ref[...] = loss.T[:8]
        sums_ref[...] = jnp.zeros_like(sums_ref)
        sums_ref[2:3, 0:LANES] = jnp.sum(loss, axis=0, keepdims=True) / count_ref[0:1, :]

        @pl.loop(0, tokens // rows)
        def _(a):
            part = pl.ds(pl.multiple_of(a * rows, rows), rows)
            h = h_ref[part, :].astype(F32)
            centred = h - jnp.mean(h, axis=-1, keepdims=True)
            inv_std = lax.rsqrt(jnp.mean(centred * centred, axis=-1, keepdims=True) + LN_EPS)
            x_hat = centred * inv_std
            d = acc_ref[part, :]
            sums_ref[0:1, :] += jnp.sum(d * x_hat, axis=0, keepdims=True)
            sums_ref[1:2, :] += jnp.sum(d, axis=0, keepdims=True)
            g = d * gain_ref[...]
            centre_term = jnp.mean(g, axis=-1, keepdims=True)
            proj_term = jnp.mean(g * x_hat, axis=-1, keepdims=True)
            dh_ref[part, :] = (inv_std * (g - centre_term - x_hat * proj_term)).astype(BF16)


def own_grad_call(order, z, e, hidden, gain, lse, info, tile, copies, rows=256):
    tokens, vocab = z.shape
    dim = e.shape[1]
    once = lambda shape: pl.BlockSpec(shape, lambda i, order: (0, 0), pipeline_mode=pl.Buffered(1))
    fixed = lambda shape: pl.BlockSpec(shape, lambda i, order: (0, 0))
    return pl.pallas_call(
        functools.partial(own_grad_body, rows, info.shape[0] * tokens // vocab),
        grid_spec=pltpu.PrefetchScalarGridSpec(
            num_scalar_prefetch=1,
            grid=(vocab // tile,),
            in_specs=[
                pl.BlockSpec((tokens, tile), lambda i, order: (0, i)),
                pl.BlockSpec((tile, dim), lambda i, order: (order[i], 0)),
                once((tokens, dim)),
                pl.BlockSpec((dim,), lambda i, order: (0,)),
                once((tokens, LANES)),
                once(info.shape),
            ],
            out_specs=[fixed((tokens, dim)), fixed((8, tokens)), fixed((copies, dim)), fixed((8, LANES))],
            scratch_shapes=[
                pltpu.VMEM((tokens, dim), F32),
                pltpu.VMEM((tokens, LANES), F32),
                pltpu.VMEM((tokens, LANES), jnp.int32),
                pltpu.VMEM((tokens, LANES), F32),
            ],
        ),
        out_shape=[
            jax.ShapeDtypeStruct((tokens, dim), BF16),
            jax.ShapeDtypeStruct((8, tokens), F32),
            jax.ShapeDtypeStruct((copies, dim), F32),
            jax.ShapeDtypeStruct((8, LANES), F32),
        ],
        compiler_params=params(),
        cost_estimate=cost(1, tokens, vocab, dim, 4 * tokens * vocab),
        name='own_grad',
    )(order, z, e, hidden, gain, lse, info)


def d_embed_body(rows, chunk, rank_ref, x_ref, e_ref, lse_ref, info_ref, count_ref, zt_ref, *refs):
    o_ref, z_buf, z_sem = refs[-3:] if len(refs) == 3 else refs[1:4]
    i = pl.program_id(0)
    last = pl.num_programs(0) - 1
    shard, width = e_ref.shape[0], x_ref.shape[0]
    fetches = [pltpu.make_async_copy(zt_ref.at[:, chunk * width:(chunk + 1) * width], z_buf, z_sem)]
    if len(refs) > 3:
        before_ref, before_buf, before_sem = refs[0], refs[4], refs[5]
        fetches.append(pltpu.make_async_copy(before_ref, before_buf, before_sem))

    @pl.when(i == 0)
    def _():
        for fetch in fetches:
            fetch.start()
        o_ref[...] = jnp.zeros_like(o_ref)

    info = info_ref[0:1, :]
    lse, tgt, w = lse_ref[0:1, :], (info >> 1) - rank_ref[0] * shard, (info & 1).astype(F32) / count_ref[0:1, 0:1]

    def part_of(r, z):
        row = lax.broadcasted_iota(jnp.int32, (rows, width), 0)
        p = jnp.exp(z - lse)
        p = jnp.where(row == tgt - r, p - 1.0, p) * w
        return jnp.dot(p.astype(BF16), x_ref[...], preferred_element_type=F32)

    @pl.when(i < last)
    def _():
        for r in range(0, shard, rows):
            z = lax.dot_general(e_ref[r:r + rows, :], x_ref[...], (((1,), (1,)), ((), ())), preferred_element_type=F32)
            o_ref[r:r + rows, :] += part_of(r, z)

    @pl.when(i == last)
    def _():
        for fetch in fetches:
            fetch.wait()

        @pl.loop(0, shard // rows)
        def _(a):
            r = pl.multiple_of(a * rows, rows)
            part = pl.ds(r, rows)
            total = o_ref[part, :] + part_of(r, z_buf[part, :])
            if len(fetches) > 1:
                total = total + before_buf[part, :]
            o_ref[part, :] = total


def d_embed_call(rank, count, x, e, lse, info, zt, before, chunk, tile, rows=256):
    tokens, dim = x.shape
    shard = e.shape[0]
    group = tokens // tile
    whose = lambda i, rank: lax.rem(rank[0] + 1 + i, group)
    stat = lambda v: pl.BlockSpec((v.shape[0] // group, tile), lambda i, rank: (whose(i, rank), chunk))
    once = lambda shape: pl.BlockSpec(shape, lambda i, rank: (0, 0), pipeline_mode=pl.Buffered(1))
    hbm = pl.BlockSpec(memory_space=pl.ANY)
    in_specs = [pl.BlockSpec((tile, dim), lambda i, rank: (whose(i, rank), 0)), once((shard, dim)), stat(lse), stat(info), once(count.shape), hbm]
    operands = [x, e, lse, info, count, zt]
    scratch = [pltpu.VMEM((shard, tile), F32), pltpu.SemaphoreType.DMA]
    if before is not None:
        in_specs.append(hbm)
        operands.append(before)
        scratch += [pltpu.VMEM((shard, dim), F32), pltpu.SemaphoreType.DMA]
    return pl.pallas_call(
        functools.partial(d_embed_body, rows, chunk),
        grid_spec=pltpu.PrefetchScalarGridSpec(
            num_scalar_prefetch=1,
            grid=(group,),
            in_specs=in_specs,
            out_specs=pl.BlockSpec((shard, dim), lambda i, rank: (0, 0)),
            scratch_shapes=scratch,
        ),
        out_shape=jax.ShapeDtypeStruct((shard, dim), F32),
        compiler_params=params(),
        cost_estimate=cost(2, tokens, shard, dim, 2 * tokens * dim + 8 * shard * dim),
        name='d_embed',
    )(rank.reshape(1), *operands)


def solution(mesh):
    group = mesh.shape['tp']

    def whole(hidden, ln_gain, ln_bias, embed, targets, loss_mask):
        tokens, dim = hidden.shape
        shard = embed.shape[0]
        rank = lax.axis_index('tp')
        copies = lambda width: -(-MIN_GATHER // (4 * group * width))
        info = lax.all_gather(jnp.tile((targets * 2 + loss_mask).reshape(1, tokens), (copies(tokens), 1)), 'tp', tiled=True)

        outs = logits_call(hidden, ln_gain, ln_bias, embed, shard * group, copies(tokens))
        lse, norms, all_embed, z, zt = outs[TOKEN_CHUNKS:]
        x_chunks = []
        for h in range(TOKEN_CHUNKS):
            x_chunks.append(lax.all_gather(outs[h], 'tp', tiled=True))
        norms = lax.all_gather(norms, 'tp', tiled=True)

        places = [place(*entry) for entry in ORDER]
        order = jnp.stack([shard_of * PIECES + n for shard_of, n in places])
        extra = -(-copies(dim) // 8) * 8
        d_hidden, loss, sums, count = own_grad_call(order, z, all_embed, hidden, ln_gain, lse, info, shard // PIECES, extra)
        sums = jnp.sum(lax.all_gather(sums, 'tp', tiled=True).reshape(group, extra, dim)[:, :3], axis=0)

        d_embed = None
        for h in range(TOKEN_CHUNKS):
            d_embed = d_embed_call(rank, count, x_chunks[h], embed, norms, info, zt, d_embed, h, tokens // TOKEN_CHUNKS)
        return loss[0], sums[2, :1], d_hidden, d_embed, sums[0], sums[1]

    token_rows = P(('dp', 'tp'))
    token_mat = P(('dp', 'tp'), None)
    return jax.shard_map(whole, mesh=mesh, in_specs=(token_mat, P(), P(), P('tp', None), token_rows, token_rows), out_specs=(token_rows, P('dp'), token_mat, token_mat, P('dp'), P('dp')), check_vma=False)
```
